32 devices in a mesh: dp: 2 (over x), tp: 16 (over y, z, core).
Axes of the slice: x: 2, y: 2, z: 4, core: 2. Of those that a mesh axis runs over, the one named last changes fastest.
Arguments:
- x: bfloat16 [5120, 7168], P(('dp', 'tp')), parts along dimension 0
- w_gate: bfloat16 [7168, 18432], P(None, 'tp')
- w_up: bfloat16 [7168, 18432], P(None, 'tp')
- w_down: bfloat16 [18432, 7168], P('tp')
Outputs:
- output: bfloat16 [5120, 7168], P(('dp', 'tp')), parts along dimension 0
There are 2 independent parts. The reference program is written for one: setup_inputs(seed, part) draws one part's arguments, and reference() takes and returns one part's arrays. A program takes and returns all parts, laid end to end along the dimension named above; an argument that names none is the same for every part.
All inputs are finite; a program needn't handle non-finite values.
Results may differ from the reference program's by a relative error of at most 0.016.
Values are sent between devices in bfloat16 or wider.
A program may use at most 2 GiB of HBM per device.

```python
import jax
import jax.numpy as jnp

ROWS = 2560
D = 7168
FF = 18432


def setup_inputs(seed: int = 0, part: int = 0) -> dict:
    kx, kg, ku, kd = jax.random.split(jax.random.key(seed), 4)
    drawn = {
        "x": jax.random.normal(jax.random.fold_in(kx, part), (ROWS, D), jnp.float32),
        "w_gate": jax.random.normal(kg, (D, FF), jnp.float32) * D**-0.5,
        "w_up": jax.random.normal(ku, (D, FF), jnp.float32) * D**-0.5,
        "w_down": jax.random.normal(kd, (FF, D), jnp.float32) * FF**-0.5,
    }
    return {k: v.astype(jnp.bfloat16) for k, v in drawn.items()}


def reference(x, w_gate, w_up, w_down):
    gate = jnp.dot(x, w_gate, preferred_element_type=jnp.float32)
    up = jnp.dot(x, w_up, preferred_element_type=jnp.float32)
    hidden = (jax.nn.silu(gate) * up).astype(jnp.bfloat16)
    return jnp.dot(hidden, w_down, preferred_element_type=jnp.float32).astype(jnp.bfloat16)
```

```python
import functools

import jax
import jax.numpy as jnp
from jax import lax
from jax.experimental import pallas as pl
from jax.experimental.pallas import tpu as pltpu
from jax.sharding import PartitionSpec as P

RING = 8
F32 = jnp.float32
BF16 = jnp.bfloat16


def chip_at(p):
    return jnp.where(p < RING // 2, p, 3 * RING // 2 - 1 - p)


def kernel(
    x_ref, wg_ref, wu_ref, wd_ref,
    y_ref, xg, tg, sg,
    w1, w2, xbuf, fbuf, hbuf, sbuf,
    wsem, lsem, xsend, xrecv, psend, precv, tsend, trecv, ssend, srecv,
):
    n = RING
    rows, dim = x_ref.shape
    half = rows // 2
    ff = wg_ref.shape[1]

    me = lax.axis_index("tp")
    core = lax.rem(me, 2)
    pos = chip_at(me // 2)

    def device(p, c):
        return {"tp": chip_at(lax.rem(p + n, n)) * 2 + c}

    down = (device(pos + 1, core), device(pos - 1, core))
    partner = device(pos, 1 - core)

    def part(d):
        return pl.ds(d * half, half)

    def remote(src, dst, send, recv, to):
        return pltpu.make_async_remote_copy(
            src_ref=src, dst_ref=dst, send_sem=send, recv_sem=recv,
            device_id=to, device_id_type=pl.DeviceIdType.MESH,
        )

    def x_first(d):
        return remote(x_ref.at[part(d)], xg.at[1, 0, part(d)], xsend.at[0, d], xrecv.at[1, d], down[d])

    def x_on(s, d):
        return remote(xg.at[s, 0, part(d)], xg.at[s + 1, 0, part(d)], xsend.at[s, d], xrecv.at[s + 1, d], down[d])

    def x_side_own(d):
        return remote(x_ref.at[part(d)], xg.at[0, 1, part(d)], psend.at[0, d], precv.at[0, d], partner)

    def x_side(s, d):
        return remote(xg.at[s, 0, part(d)], xg.at[s, 1, part(d)], psend.at[s, d], precv.at[s, d], partner)

    def term_side(s):
        return remote(xbuf.at[pl.ds(0, rows)], tg.at[s], tsend.at[s], trecv.at[s], partner)

    def sum_on(s, d):
        return remote(sbuf.at[part(d)], sg.at[s + 1, part(d)], ssend.at[s, d], srecv.at[s + 1, d], down[d])

    def weights():
        return (
            pltpu.make_async_copy(wg_ref, w1.at[:, pl.ds(0, ff)], wsem.at[0]),
            pltpu.make_async_copy(wu_ref, w1.at[:, pl.ds(ff, ff)], wsem.at[1]),
            pltpu.make_async_copy(wd_ref, w2, wsem.at[2]),
        )

    barrier = pltpu.get_barrier_semaphore()
    for other in (*down, partner):
        pl.semaphore_signal(barrier, inc=1, device_id=other, device_id_type=pl.DeviceIdType.MESH)
    pl.semaphore_wait(barrier, 3)

    for d in range(2):
        x_first(d).start()
    for d in range(2):
        x_side_own(d).start()
    for copy in weights():
        copy.start()
    for copy in weights():
        copy.wait()

    n1 = 768
    n2 = 512
    wide = fbuf.shape[1]
    per = wide // n2
    low = pl.ds(0, rows)
    high = pl.ds(rows, rows)

    def step(s, carry):
        slot = lax.rem(s, n)

        @pl.when(s < n)
        def _():
            for d in range(2):
                x_on(s - 1, d).wait_recv()

        @pl.when(s < n - 1)
        def _():
            for d in range(2):
                x_on(s, d).start()

        @pl.when(s > 1)
        def _():
            term_side(s - 1).wait_send()

        own_copy = pltpu.make_async_copy(xg.at[slot, 0], xbuf.at[low], lsem.at[0])

        @pl.when(s < n)
        def _():
            for d in range(2):
                x_side(s, d).start()
            own_copy.start()

        @pl.when(s == n)
        def _():
            pltpu.make_async_copy(x_ref, xbuf.at[low], lsem.at[0]).start()

        for d in range(2):
            x_side(slot, d).wait_recv()
        side_copy = pltpu.make_async_copy(xg.at[slot, 1], xbuf.at[high], lsem.at[1])
        side_copy.start()
        own_copy.wait()
        side_copy.wait()

        def first(j, c):
            cols = pl.ds(pl.multiple_of(j * n1, n1), n1)
            fbuf[:, cols] = jnp.dot(xbuf[...], w1[:, cols], preferred_element_type=F32)
            return c

        lax.fori_loop(0, 2 * ff // n1, first, 0)

        def gated(j, c):
            at = pl.ds(pl.multiple_of(j * 32, 32), 32)
            gate = fbuf[at, pl.ds(0, ff)]
            up = fbuf[at, pl.ds(ff, ff)]
            hbuf[at, :] = (jax.nn.silu(gate) * up).astype(BF16)
            return c

        lax.fori_loop(0, 2 * rows // 32, gated, 0)

        def second(j, c):
            cols = pl.ds(pl.multiple_of(j * n2, n2), n2)
            term = jnp.dot(hbuf[...], w2[:, cols], preferred_element_type=F32)
            at = pl.ds(pl.multiple_of((j // per) * rows, rows), rows)
            fcols = pl.ds(pl.multiple_of(lax.rem(j, per) * n2, n2), n2)
            fbuf[at, fcols] = term[:rows]
            xbuf[low, cols] = term[rows:].astype(BF16)
            return c

        lax.fori_loop(0, dim // n2, second, 0)

        term_side(s).start()

        @pl.when(s == 1)
        def _():
            def clear(j, c):
                cols = pl.ds(pl.multiple_of(j * n2, n2), n2)
                sbuf[:, cols] = jnp.zeros((rows, n2), BF16)
                return c

            lax.fori_loop(0, dim // n2, clear, 0)

        term_side(s).wait_recv()
        term_copy = pltpu.make_async_copy(tg.at[s], xbuf.at[high], lsem.at[0])
        term_copy.start()

        def sum_copy(d):
            return pltpu.make_async_copy(sg.at[s, part(d)], sbuf.at[part(d)], lsem.at[2 + d])

        @pl.when(s > 1)
        def _():
            for d in range(2):
                sum_on(s - 1, d).wait_recv()
                sum_on(s - 1, d).wait_send()
                sum_copy(d).start()

        term_copy.wait()
        for d in range(2):
            @pl.when(s > 1)
            def _():
                sum_copy(d).wait()

            def add(j, c):
                cols = pl.ds(pl.multiple_of(j * n2, n2), n2)
                at = pl.ds(pl.multiple_of((j // per) * rows + d * half, half), half)
                fcols = pl.ds(pl.multiple_of(lax.rem(j, per) * n2, n2), n2)
                total = fbuf[at, fcols] + xbuf[pl.ds(rows + d * half, half), cols].astype(F32)
                sbuf[part(d), cols] = (total + sbuf[part(d), cols].astype(F32)).astype(BF16)
                return c

            lax.fori_loop(0, dim // n2, add, 0)

            @pl.when(s < n)
            def _():
                sum_on(s, d).start()

            @pl.when(s == n)
            def _():
                pltpu.make_async_copy(sbuf.at[part(d)], y_ref.at[part(d)], lsem.at[2 + d]).start()

        return carry

    lax.fori_loop(1, n + 1, step, 0)

    for d in range(2):
        pltpu.make_async_copy(sbuf.at[part(d)], y_ref.at[part(d)], lsem.at[2 + d]).wait()
    term_side(n).wait_send()
    for d in range(2):
        x_first(d).wait_send()
        x_side_own(d).wait_send()

    def drain(s, c):
        for d in range(2):
            x_side(s, d).wait_send()

            @pl.when(s < n - 1)
            def _():
                x_on(s, d).wait_send()
        return c

    lax.fori_loop(1, n, drain, 0)


def solution(mesh):
    assert mesh.shape["tp"] == 2 * RING

    def step(x, w_gate, w_up, w_down):
        rows, dim = x.shape
        ff = w_gate.shape[1]
        n = RING
        hbm = pl.BlockSpec(memory_space=pl.ANY)
        dma = pltpu.SemaphoreType.DMA
        outs = pl.pallas_call(
            kernel,
            out_shape=[
                jax.ShapeDtypeStruct((rows, dim), BF16),
                jax.ShapeDtypeStruct((n, 2, rows, dim), BF16),
                jax.ShapeDtypeStruct((n + 1, rows, dim), BF16),
                jax.ShapeDtypeStruct((n + 1, rows, dim), BF16),
            ],
            in_specs=[hbm] * 4,
            out_specs=[hbm] * 4,
            scratch_shapes=[
                pltpu.VMEM((dim, 2 * ff), BF16),
                pltpu.VMEM((ff, dim), BF16),
                pltpu.VMEM((2 * rows, dim), BF16),
                pltpu.VMEM((2 * rows, dim // 2), F32),
                pltpu.VMEM((2 * rows, ff), BF16),
                pltpu.VMEM((rows, dim), BF16),
                dma((3,)),
                dma((4,)),
                dma((n, 2)),
                dma((n, 2)),
                dma((n, 2)),
                dma((n, 2)),
                dma((n + 1,)),
                dma((n + 1,)),
                dma((n + 1, 2)),
                dma((n + 1, 2)),
            ],
            compiler_params=pltpu.CompilerParams(
                collective_id=0, has_side_effects=True, vmem_limit_bytes=67043328
            ),
        )(x, w_gate, w_up, w_down)
        return outs[0]

    return jax.shard_map(
        step,
        mesh=mesh,
        in_specs=(P(("dp", "tp"), None), P(None, "tp"), P(None, "tp"), P("tp", None)),
        out_specs=P(("dp", "tp"), None),
        check_vma=False,
    )
```

```python
import jax
import jax.numpy as jnp
from jax import lax
from jax.experimental import pallas as pl
from jax.experimental.pallas import tpu as pltpu
from jax.sharding import PartitionSpec as P

RING = 8
CHUNK = 16
K1 = 3584
N1 = 768
N2 = 1024
OWN_STEP = 3
F32 = jnp.float32
BF16 = jnp.bfloat16

X_TO = [['n', 'n', 'n', '', 'n', '', '', ''], ['nm', 'n', 'mn', 'n', '', 'n', 'p', 'p'], ['n', 'nm', 'n', 'n', 'mn', 'n', 'n', 'p'], ['n', 'n', 'n', 'n', '', '', 'n', '']]
S_MID = [[0, 0, 0, 0, 0, 0, 0], [1, 0, 0, 0, 0, 0, 0], [1, 1, 1, 1, 0, 0, 0], [0, 0, 0, 0, 0, 0, 0]]
IN_PREV = [[0, 1, 1, 1, 1, 1, 1, 1], [0, 1, 1, 1, 1, 1, 1, 1], [0, 0, 1, 1, 1, 1, 1, 1], [0, 0, 0, 0, 0, 1, 1, 1]]
IN_MID = [[0, 0, 0, 0, 0, 0, 0, 0], [0, 0, 0, 1, 1, 1, 1, 0], [0, 0, 0, 0, 0, 1, 0, 0], [0, 0, 0, 0, 0, 0, 0, 0]]
SERVE = [[0, 1, 3, 5, 7, 8, 10], [0, 1, 3, 5, 7, 5, 6], [0, 1, 3, 3, 2, 9, 3], [0, 1, 3, 5, 6, 7, 11]]


def chip_at(p):
    return jnp.where(p < RING // 2, p, 3 * RING // 2 - 1 - p)


def kernel(
    x_ref, wg_ref, wu_ref, wd_ref,
    y_ref, xg, tg, sg, hsave,
    w1, w2, xbuf, fbuf, gbuf, hbuf, sbuf,
    wsem, lsem, hsem, csem, xsend, xrecv, psend, precv, tsend, trecv, ssend, srecv,
):
    n = RING
    rows, dim = x_ref.shape
    half = rows // 2
    ff = wg_ref.shape[1]
    chunks = half // CHUNK

    me = lax.axis_index("tp")
    core = lax.rem(me, 2)
    pos = chip_at(me // 2)
    roles = (pos, n - 1 - pos)
    classes = tuple(lax.rem(q, 4) for q in roles)

    def device(p, c):
        return {"tp": chip_at(lax.rem(p + n, n)) * 2 + c}

    ahead = (device(pos + 1, core), device(pos - 1, core))
    behind = (ahead[1], ahead[0])
    across = device(n - 1 - pos, core)
    partner = device(pos, 1 - core)
    low = pl.ds(0, rows)
    high = pl.ds(rows, rows)

    def at(d, i):
        return pl.ds(pl.multiple_of(d * half + i * CHUNK, CHUNK), CHUNK)

    def any_class(d, flags):
        cond = None
        for c, flag in enumerate(flags):
            if flag:
                cond = (classes[d] == c) if cond is None else cond | (classes[d] == c)
        return cond

    def any_pair(d, s, table):
        cond = None
        for c, row in enumerate(table):
            for o, flag in enumerate(row):
                if flag:
                    hit = (classes[d] == c) & (s == o + 1)
                    cond = hit if cond is None else cond | hit
        return cond

    def across_at(d, o):
        return lax.rem(3 * n - 1 - 2 * roles[d] + o, n)

    def remote(src, dst, send, recv, to):
        return pltpu.make_async_remote_copy(
            src_ref=src, dst_ref=dst, send_sem=send, recv_sem=recv,
            device_id=to, device_id_type=pl.DeviceIdType.MESH,
        )

    def x_copy(o, d, i, kind):
        src = x_ref if o == 0 else xg.at[o, 0]
        slot = {"n": o + 1, "p": (o - 1) % n, "m": across_at(d, o)}[kind]
        to = {"n": ahead[d], "p": behind[d], "m": across}[kind]
        return remote(
            src.at[at(d, i)], xg.at[slot, 0, at(d, i)], xsend.at[o, "npm".index(kind), d, i], xrecv.at[slot, d, i], to
        )

    def x_arrived(o, d, i):
        return remote(xg.at[o, 0, at(d, i)], xg.at[o, 0, at(d, i)], xsend.at[o, 0, d, i], xrecv.at[o, d, i], ahead[d])

    def x_on(o, d, i, active, act):
        for kind in "npm":
            flags = [kind in X_TO[c][o] for c in range(4)]
            if not any(flags):
                continue
            cond = any_class(d, flags)

            @pl.when(cond if active is None else cond & active)
            def _():
                act(x_copy(o, d, i, kind))

    def x_side_own():
        return remote(x_ref, xg.at[0, 1], psend.at[0, 0, 0], precv.at[0, 0, 0], partner)

    def x_side(o, d, i):
        return remote(xg.at[o, 0, at(d, i)], xg.at[o, 1, at(d, i)], psend.at[o, d, i], precv.at[o, d, i], partner)

    def term_side(s, j):
        cols = pl.ds(pl.multiple_of(j * N2, N2), N2)
        return remote(xbuf.at[low, cols], tg.at[s, :, cols], tsend, trecv.at[s], partner)

    def term_all(s):
        return remote(xbuf.at[low], tg.at[s], tsend, trecv.at[s], partner)

    def out(s, d, i):
        return sbuf.at[lax.rem(s, 2), at(d, i)]

    def sum_copy(s, d, i, mid):
        if mid:
            slot = across_at(d, s)
            slot = jnp.where(slot == 0, n, slot)
            return remote(out(s, d, i), sg.at[slot, 1, at(d, i)], ssend.at[s, d, i], srecv.at[slot, 1, d, i], across)
        return remote(out(s, d, i), sg.at[s + 1, 0, at(d, i)], ssend.at[s, d, i], srecv.at[s + 1, 0, d, i], ahead[d])

    def sum_arrived(s, k, d, i):
        ref = sg.at[s, k, at(d, i)]
        return remote(ref, ref, ssend.at[s, d, i], srecv.at[s, k, d, i], ahead[d])

    def each(body):
        def go(i, c):
            body(i)
            return c

        lax.fori_loop(0, chunks, go, 0)

    tiles = 2 * ff // N1
    sub = N1 // 2

    def up_weights():
        out = []
        for j in range(tiles):
            src = pl.ds(j * sub, sub)
            out.append(pltpu.make_async_copy(wg_ref.at[:, src], w1.at[:, pl.ds(j * N1, sub)], wsem.at[2 * j]))
            out.append(pltpu.make_async_copy(wu_ref.at[:, src], w1.at[:, pl.ds(j * N1 + sub, sub)], wsem.at[2 * j + 1]))
        return out

    def down_weights():
        return pltpu.make_async_copy(wd_ref, w2, wsem.at[2 * tiles])

    def gate_up():
        def first(t, c):
            j, m = t // 2, lax.rem(t, 2)
            mine = pl.ds(pl.multiple_of(m * rows, rows), rows)
            cols = pl.ds(pl.multiple_of(j * N1, N1), N1)
            gbuf[...] = jnp.dot(xbuf[mine, :K1], w1[:K1, cols], preferred_element_type=F32)

            def deeper(k, c):
                ks = pl.ds(pl.multiple_of(k * K1, K1), K1)
                gbuf[...] += jnp.dot(xbuf[mine, ks], w1[ks, cols], preferred_element_type=F32)
                return c

            lax.fori_loop(1, dim // K1, deeper, 0)
            to = pl.ds(pl.multiple_of(j * sub, sub), sub)

            def gated(r, c):
                rs = pl.ds(pl.multiple_of(r * 32, 32), 32)
                ro = pl.ds(pl.multiple_of(m * rows + r * 32, 32), 32)
                hbuf[ro, to] = (jax.nn.silu(gbuf[rs, pl.ds(0, sub)]) * gbuf[rs, pl.ds(sub, sub)]).astype(BF16)
                return c

            return lax.fori_loop(0, rows // 32, gated, c)

        lax.fori_loop(0, 2 * tiles, first, 0)

    def project(s, between):
        def second(j, c):
            cols = pl.ds(pl.multiple_of(j * N2, N2), N2)
            term = jnp.dot(hbuf[...], w2[:, cols], preferred_element_type=F32)
            fbuf[:, cols] = term[:rows]
            xbuf[low, cols] = term[rows:].astype(BF16)
            term_side(s, j).start()
            return c

        lax.fori_loop(0, dim // N2, second, 0)
        between()
        term_all(s).wait_send()

    def serve(point):
        for o in range(1, n):
            for d in range(2):
                active = None
                for c in range(4):
                    hit = (classes[d] == c) & (point == SERVE[c][o - 1])
                    active = hit if active is None else active | hit

                @pl.when(active)
                def _():
                    def body(i):
                        x_arrived(o, d, i).wait_recv()
                        x_on(o, d, i, None, lambda copy: copy.start())
                        x_side(o, d, i).start()

                    each(body)

    def own_load(s):
        return pltpu.make_async_copy(xg.at[s, 0], xbuf.at[low], lsem.at[0])

    def load_x(s):
        own_load(s).start()

        def body(i):
            for d in range(2):
                x_side(s, d, i).wait_recv()

        each(body)
        side = pltpu.make_async_copy(xg.at[s, 1], xbuf.at[high], lsem.at[1])
        side.start()
        own_load(s).wait()
        side.wait()

    def term_load(s):
        return pltpu.make_async_copy(tg.at[s], xbuf.at[high], lsem.at[0])

    def add_on(s):
        comes = [(any_pair(d, s, IN_PREV), any_pair(d, s, IN_MID)) for d in range(2)]
        crosses = [any_pair(d, s, S_MID) for d in range(2)]

        def fold(j, c):
            cols = pl.ds(pl.multiple_of(j * N2, N2), N2)
            fbuf[:, cols] += xbuf[high, cols].astype(F32)
            return c

        term_load(s).wait()
        lax.fori_loop(0, dim // N2, fold, 0)

        def under(d, i):
            return pl.ds(pl.multiple_of(rows + d * half + i * CHUNK, CHUNK), CHUNK)

        def body(i):
            def staged(d):
                return (
                    pltpu.make_async_copy(sg.at[s, 0, at(d, i)], xbuf.at[at(d, i)], csem.at[d, 0]),
                    pltpu.make_async_copy(sg.at[s, 1, at(d, i)], xbuf.at[under(d, i)], csem.at[d, 1]),
                )

            for d in range(2):
                @pl.when(comes[d][1])
                def _():
                    sum_arrived(s, 1, d, i).wait_recv()
                    staged(d)[1].start()

                @pl.when(comes[d][0])
                def _():
                    sum_arrived(s, 0, d, i).wait_recv()
                    staged(d)[0].start()

            for d in range(2):
                @pl.when(s > 2)
                def _():
                    sum_copy(s - 2, d, i, False).wait_send()

                @pl.when(comes[d][1])
                def _():
                    staged(d)[1].wait()
                    fbuf[at(d, i), :] += xbuf[under(d, i), :].astype(F32)

                @pl.when(comes[d][0])
                def _():
                    staged(d)[0].wait()
                    out(s, d, i)[...] = (fbuf[at(d, i), :] + xbuf[at(d, i), :].astype(F32)).astype(BF16)

                @pl.when(jnp.logical_not(comes[d][0]))
                def _():
                    out(s, d, i)[...] = fbuf[at(d, i), :].astype(BF16)

                @pl.when((s < n) & crosses[d])
                def _():
                    sum_copy(s, d, i, True).start()

                @pl.when((s < n) & jnp.logical_not(crosses[d]))
                def _():
                    sum_copy(s, d, i, False).start()

                @pl.when(s == n)
                def _():
                    y_copy(d, i).start()

        each(body)

    def y_copy(d, i):
        return pltpu.make_async_copy(out(n, d, i), y_ref.at[at(d, i)], ssend.at[n, d, i])

    barrier = pltpu.get_barrier_semaphore()
    for other in (*ahead, across, partner):
        pl.semaphore_signal(barrier, inc=1, device_id=other, device_id_type=pl.DeviceIdType.MESH)
    pl.semaphore_wait(barrier, 4)

    def send_first(i):
        for d in range(2):
            x_on(0, d, i, None, lambda copy: copy.start())

    each(send_first)
    x_side_own().start()
    for copy in up_weights():
        copy.start()
    down_weights().start()
    serve(0)
    load_x(1)
    for copy in up_weights():
        copy.wait()
    gate_up()
    down_weights().wait()

    def saved(to_hbm):
        if to_hbm:
            return pltpu.make_async_copy(hbuf, hsave, hsem)
        return pltpu.make_async_copy(hsave, hbuf, hsem)

    def step(s, carry):
        @pl.when((s > 0) & (s < n - 1))
        def _():
            load_x(s + 1)
            gate_up()

        @pl.when(s == n - 1)
        def _():
            saved(False).start()
            saved(False).wait()

        @pl.when(s > 0)
        def _():
            term_all(s).wait_recv()
            term_load(s).start()
            serve(2 * s)
            add_on(s)

        @pl.when(s < n)
        def _():
            project(s + 1, lambda: serve(2 * s + 1))

        @pl.when(s == OWN_STEP)
        def _():
            own = pltpu.make_async_copy(x_ref, xbuf.at[low], lsem.at[0])
            own.start()
            x_side_own().wait_recv()
            side = pltpu.make_async_copy(xg.at[0, 1], xbuf.at[high], lsem.at[1])
            side.start()
            own.wait()
            side.wait()
            gate_up()
            saved(True).start()
            saved(True).wait()

        return carry

    lax.fori_loop(0, n + 1, step, 0)

    def finish(i):
        for d in range(2):
            for o in range(n):
                x_on(o, d, i, None, lambda copy: copy.wait_send())
                if o:
                    x_side(o, d, i).wait_send()
            sum_copy(n - 1, d, i, False).wait_send()
            y_copy(d, i).wait()

    each(finish)
    x_side_own().wait_send()


def solution(mesh):
    assert mesh.shape["tp"] == 2 * RING

    def step(x, w_gate, w_up, w_down):
        rows, dim = x.shape
        ff = w_gate.shape[1]
        n = RING
        chunks = rows // 2 // CHUNK
        hbm = pl.BlockSpec(memory_space=pl.ANY)
        dma = pltpu.SemaphoreType.DMA
        outs = pl.pallas_call(
            kernel,
            out_shape=[
                jax.ShapeDtypeStruct((rows, dim), BF16),
                jax.ShapeDtypeStruct((n, 2, rows, dim), BF16),
                jax.ShapeDtypeStruct((n + 1, rows, dim), BF16),
                jax.ShapeDtypeStruct((n + 1, 2, rows, dim), BF16),
                jax.ShapeDtypeStruct((2 * rows, ff), BF16),
            ],
            in_specs=[hbm] * 4,
            out_specs=[hbm] * 5,
            scratch_shapes=[
                pltpu.VMEM((dim, 2 * ff), BF16),
                pltpu.VMEM((ff, dim), BF16),
                pltpu.VMEM((2 * rows, dim), BF16),
                pltpu.VMEM((rows, dim), F32),
                pltpu.VMEM((rows, N1), F32),
                pltpu.VMEM((2 * rows, ff), BF16),
                pltpu.VMEM((2, rows, dim), BF16),
                dma((4 * ff // N1 + 1,)),
                dma((2,)),
                dma,
                dma((2, 2)),
                dma((n, 3, 2, chunks)),
                dma((n, 2, chunks)),
                dma((n, 2, chunks)),
                dma((n, 2, chunks)),
                dma,
                dma((n + 1,)),
                dma((n + 1, 2, chunks)),
                dma((n + 1, 2, 2, chunks)),
            ],
            compiler_params=pltpu.CompilerParams(
                collective_id=0, has_side_effects=True, vmem_limit_bytes=67043328
            ),
        )(x, w_gate, w_up, w_down)
        return outs[0]

    return jax.shard_map(
        step,
        mesh=mesh,
        in_specs=(P(("dp", "tp"), None), P(None, "tp"), P(None, "tp"), P("tp", None)),
        out_specs=P(("dp", "tp"), None),
        check_vma=False,
    )
```

```python
import jax
import jax.numpy as jnp
from jax import lax
from jax.experimental import pallas as pl
from jax.experimental.pallas import tpu as pltpu
from jax.sharding import PartitionSpec as P

RING = 8
CHUNK = 16
K1 = 3584
N1 = 768
N2 = 1024
OWN_STEP = 3
F32 = jnp.float32
BF16 = jnp.bfloat16

X_TO = [['n', 'n', 'n', '', 'n', '', '', ''], ['nm', 'n', 'mn', 'n', '', 'n', 'p', 'p'], ['n', 'nm', 'n', 'n', 'mn', 'n', 'n', 'p'], ['n', 'n', 'n', 'n', '', '', 'n', '']]
S_MID = [[0, 0, 0, 0, 0, 0, 0], [1, 1, 0, 0, 0, 0, 0], [1, 1, 1, 1, 1, 0, 0], [0, 0, 0, 0, 0, 0, 0]]
IN_PREV = [[0, 1, 1, 1, 1, 1, 1, 1], [0, 1, 1, 1, 1, 1, 1, 1], [0, 0, 0, 1, 1, 1, 1, 1], [0, 0, 0, 0, 0, 0, 1, 1]]
IN_MID = [[0, 0, 0, 0, 0, 0, 0, 0], [0, 0, 0, 1, 1, 1, 1, 1], [0, 0, 0, 0, 0, 1, 1, 0], [0, 0, 0, 0, 0, 0, 0, 0]]
SERVE = [[2, 3, 7, 12, 16, 20, 24], [2, 3, 7, 6, 16, 13, 15], [2, 3, 8, 10, 3, 20, 7], [2, 3, 8, 12, 15, 15, 24]]


def chip_at(p):
    return jnp.where(p < RING // 2, p, 3 * RING // 2 - 1 - p)


def kernel(
    x_ref, wg_ref, wu_ref, wd_ref,
    y_ref, xg, tg, sg, hsave,
    w1, w2, xbuf, fbuf, gbuf, hbuf, sbuf,
    wsem, lsem, hsem, csem, xsend, xrecv, psend, precv, tsend, trecv, ssend, srecv,
):
    n = RING
    rows, dim = x_ref.shape
    half = rows // 2
    ff = wg_ref.shape[1]
    chunks = half // CHUNK

    me = lax.axis_index("tp")
    core = lax.rem(me, 2)
    pos = chip_at(me // 2)
    roles = (pos, n - 1 - pos)
    classes = tuple(lax.rem(q, 4) for q in roles)

    def device(p, c):
        return {"tp": chip_at(lax.rem(p + n, n)) * 2 + c}

    ahead = (device(pos + 1, core), device(pos - 1, core))
    behind = (ahead[1], ahead[0])
    across = device(n - 1 - pos, core)
    partner = device(pos, 1 - core)
    low = pl.ds(0, rows)
    high = pl.ds(rows, rows)

    def at(d, i):
        return pl.ds(pl.multiple_of(d * half + i * CHUNK, CHUNK), CHUNK)

    def any_class(d, flags):
        cond = None
        for c, flag in enumerate(flags):
            if flag:
                cond = (classes[d] == c) if cond is None else cond | (classes[d] == c)
        return cond

    def any_pair(d, s, table):
        cond = None
        for c, row in enumerate(table):
            for o, flag in enumerate(row):
                if flag:
                    hit = (classes[d] == c) & (s == o + 1)
                    cond = hit if cond is None else cond | hit
        return cond

    def across_at(d, o):
        return lax.rem(3 * n - 1 - 2 * roles[d] + o, n)

    def remote(src, dst, send, recv, to):
        return pltpu.make_async_remote_copy(
            src_ref=src, dst_ref=dst, send_sem=send, recv_sem=recv,
            device_id=to, device_id_type=pl.DeviceIdType.MESH,
        )

    def x_copy(o, d, i, kind):
        src = x_ref if o == 0 else xg.at[o, 0]
        slot = {"n": o + 1, "p": (o - 1) % n, "m": across_at(d, o)}[kind]
        to = {"n": ahead[d], "p": behind[d], "m": across}[kind]
        return remote(
            src.at[at(d, i)], xg.at[slot, 0, at(d, i)], xsend.at[o, "npm".index(kind), d, i], xrecv.at[slot, d, i], to
        )

    def x_arrived(o, d, i):
        return remote(xg.at[o, 0, at(d, i)], xg.at[o, 0, at(d, i)], xsend.at[o, 0, d, i], xrecv.at[o, d, i], ahead[d])

    def x_on(o, d, i, active, act):
        for kind in "npm":
            flags = [kind in X_TO[c][o] for c in range(4)]
            if not any(flags):
                continue
            cond = any_class(d, flags)

            @pl.when(cond if active is None else cond & active)
            def _():
                act(x_copy(o, d, i, kind))

    def x_side_own():
        return remote(x_ref, xg.at[0, 1], psend.at[0, 0, 0], precv.at[0, 0, 0], partner)

    def x_side(o, d, i):
        return remote(xg.at[o, 0, at(d, i)], xg.at[o, 1, at(d, i)], psend.at[o, d, i], precv.at[o, d, i], partner)

    def term_side(s, j):
        cols = pl.ds(pl.multiple_of(j * N2, N2), N2)
        return remote(xbuf.at[low, cols], tg.at[s, :, cols], tsend, trecv.at[s], partner)

    def term_all(s):
        return remote(xbuf.at[low], tg.at[s], tsend, trecv.at[s], partner)

    def out(s, d, i):
        return sbuf.at[lax.rem(s, 2), at(d, i)]

    def sum_copy(s, d, i, mid):
        if mid:
            slot = across_at(d, s)
            slot = jnp.where(slot == 0, n, slot)
            return remote(out(s, d, i), sg.at[slot, 1, at(d, i)], ssend.at[s, d, i], srecv.at[slot, 1, d, i], across)
        return remote(out(s, d, i), sg.at[s + 1, 0, at(d, i)], ssend.at[s, d, i], srecv.at[s + 1, 0, d, i], ahead[d])

    def sum_arrived(s, k, d, i):
        ref = sg.at[s, k, at(d, i)]
        return remote(ref, ref, ssend.at[s, d, i], srecv.at[s, k, d, i], ahead[d])

    def each(body):
        def go(i, c):
            body(i)
            return c

        lax.fori_loop(0, chunks, go, 0)

    tiles = 2 * ff // N1
    sub = N1 // 2

    def up_weights():
        out = []
        for j in range(tiles):
            src = pl.ds(j * sub, sub)
            out.append(pltpu.make_async_copy(wg_ref.at[:, src], w1.at[:, pl.ds(j * N1, sub)], wsem.at[2 * j]))
            out.append(pltpu.make_async_copy(wu_ref.at[:, src], w1.at[:, pl.ds(j * N1 + sub, sub)], wsem.at[2 * j + 1]))
        return out

    def down_weights():
        return pltpu.make_async_copy(wd_ref, w2, wsem.at[2 * tiles])

    def gate_up(late=None, halfway=None):
        def first(t, c):
            j, m = lax.rem(t, tiles), t // tiles
            if late is not None:
                pl.when(t == tiles)(lambda: side_load(late).wait())
            mine = pl.ds(pl.multiple_of(m * rows, rows), rows)
            cols = pl.ds(pl.multiple_of(j * N1, N1), N1)
            gbuf[...] = jnp.dot(xbuf[mine, :K1], w1[:K1, cols], preferred_element_type=F32)

            def deeper(k, c):
                ks = pl.ds(pl.multiple_of(k * K1, K1), K1)
                gbuf[...] += jnp.dot(xbuf[mine, ks], w1[ks, cols], preferred_element_type=F32)
                return c

            lax.fori_loop(1, dim // K1, deeper, 0)
            to = pl.ds(pl.multiple_of(j * sub, sub), sub)

            def gated(r, c):
                rs = pl.ds(pl.multiple_of(r * 32, 32), 32)
                ro = pl.ds(pl.multiple_of(m * rows + r * 32, 32), 32)
                hbuf[ro, to] = (jax.nn.silu(gbuf[rs, pl.ds(0, sub)]) * gbuf[rs, pl.ds(sub, sub)]).astype(BF16)
                return c

            lax.fori_loop(0, rows // 32, gated, 0)
            if late is not None:
                pl.when(t == 0)(lambda: side_start(late))
            if halfway is not None:
                pl.when(t == tiles - 1)(halfway)
            return c

        lax.fori_loop(0, 2 * tiles, first, 0)

    def project(s, between):
        def second(j, c):
            cols = pl.ds(pl.multiple_of(j * N2, N2), N2)
            term = jnp.dot(hbuf[...], w2[:, cols], preferred_element_type=F32)
            fbuf[:, cols] = term[:rows]
            xbuf[low, cols] = term[rows:].astype(BF16)
            term_side(s, j).start()
            return c

        lax.fori_loop(0, dim // N2, second, 0)
        between()
        term_all(s).wait_send()

    def serve(point):
        for o in range(1, n):
            for d in range(2):
                active = None
                for c in range(4):
                    hit = (classes[d] == c) & (point == SERVE[c][o - 1])
                    active = hit if active is None else active | hit

                @pl.when(active)
                def _():
                    def body(i):
                        x_arrived(o, d, i).wait_recv()
                        x_on(o, d, i, None, lambda copy: copy.start())
                        x_side(o, d, i).start()

                    each(body)

    def own_load(s):
        return pltpu.make_async_copy(xg.at[s, 0], xbuf.at[low], lsem.at[0])

    def side_load(s):
        return pltpu.make_async_copy(xg.at[s, 1], xbuf.at[high], lsem.at[1])

    def side_start(s):
        def body(i):
            for d in range(2):
                x_side(s, d, i).wait_recv()

        each(body)
        side_load(s).start()

    def load_x(s):
        own_load(s).start()
        own_load(s).wait()

    def term_load(s):
        return pltpu.make_async_copy(tg.at[s], xbuf.at[high], lsem.at[0])

    def add_on(s):
        comes = [(any_pair(d, s, IN_PREV), any_pair(d, s, IN_MID)) for d in range(2)]
        crosses = [any_pair(d, s, S_MID) for d in range(2)]

        def fold(j, c):
            cols = pl.ds(pl.multiple_of(j * N2, N2), N2)
            fbuf[:, cols] += xbuf[high, cols].astype(F32)
            return c

        term_load(s).wait()
        lax.fori_loop(0, dim // N2, fold, 0)

        def under(d, i):
            return pl.ds(pl.multiple_of(rows + d * half + i * CHUNK, CHUNK), CHUNK)

        def body(i):
            def staged(d):
                return (
                    pltpu.make_async_copy(sg.at[s, 0, at(d, i)], xbuf.at[at(d, i)], csem.at[d, 0]),
                    pltpu.make_async_copy(sg.at[s, 1, at(d, i)], xbuf.at[under(d, i)], csem.at[d, 1]),
                )

            for d in range(2):
                @pl.when(comes[d][1])
                def _():
                    sum_arrived(s, 1, d, i).wait_recv()
                    staged(d)[1].start()

                @pl.when(comes[d][0])
                def _():
                    sum_arrived(s, 0, d, i).wait_recv()
                    staged(d)[0].start()

            for d in range(2):
                @pl.when(s > 2)
                def _():
                    sum_copy(s - 2, d, i, False).wait_send()

                @pl.when(comes[d][1])
                def _():
                    staged(d)[1].wait()
                    fbuf[at(d, i), :] += xbuf[under(d, i), :].astype(F32)

                @pl.when(comes[d][0])
                def _():
                    staged(d)[0].wait()
                    out(s, d, i)[...] = (fbuf[at(d, i), :] + xbuf[at(d, i), :].astype(F32)).astype(BF16)

                @pl.when(jnp.logical_not(comes[d][0]))
                def _():
                    out(s, d, i)[...] = fbuf[at(d, i), :].astype(BF16)

                @pl.when((s < n) & crosses[d])
                def _():
                    sum_copy(s, d, i, True).start()

                @pl.when((s < n) & jnp.logical_not(crosses[d]))
                def _():
                    sum_copy(s, d, i, False).start()

                @pl.when(s == n)
                def _():
                    y_copy(d, i).start()

        each(body)

    def y_copy(d, i):
        return pltpu.make_async_copy(out(n, d, i), y_ref.at[at(d, i)], ssend.at[n, d, i])

    barrier = pltpu.get_barrier_semaphore()
    for other in (*ahead, across, partner):
        pl.semaphore_signal(barrier, inc=1, device_id=other, device_id_type=pl.DeviceIdType.MESH)
    pl.semaphore_wait(barrier, 4)

    def send_first(i):
        for d in range(2):
            x_on(0, d, i, None, lambda copy: copy.start())

    each(send_first)
    x_side_own().start()
    for copy in up_weights():
        copy.start()
    down_weights().start()
    serve(2)
    load_x(1)
    for copy in up_weights():
        copy.wait()
    gate_up(1)
    down_weights().wait()

    def saved(to_hbm):
        if to_hbm:
            return pltpu.make_async_copy(hbuf, hsave, hsem)
        return pltpu.make_async_copy(hsave, hbuf, hsem)

    def step(s, carry):
        @pl.when((s > 0) & (s < n - 1))
        def _():
            serve(4 * s)
            load_x(s + 1)
            gate_up(s + 1, lambda: serve(4 * s + 1))

        @pl.when(s == n - 1)
        def _():
            saved(False).start()
            saved(False).wait()

        @pl.when(s > 0)
        def _():
            term_all(s).wait_recv()
            term_load(s).start()
            serve(4 * s + 2)
            add_on(s)

        @pl.when(s < n)
        def _():
            project(s + 1, lambda: serve(4 * s + 3))

        @pl.when(s == OWN_STEP)
        def _():
            own = pltpu.make_async_copy(x_ref, xbuf.at[low], lsem.at[0])
            own.start()
            x_side_own().wait_recv()
            side = pltpu.make_async_copy(xg.at[0, 1], xbuf.at[high], lsem.at[1])
            side.start()
            own.wait()
            side.wait()
            gate_up()
            saved(True).start()
            saved(True).wait()

        return carry

    lax.fori_loop(0, n + 1, step, 0)

    def finish(i):
        for d in range(2):
            for o in range(n):
                x_on(o, d, i, None, lambda copy: copy.wait_send())
                if o:
                    x_side(o, d, i).wait_send()
            sum_copy(n - 1, d, i, False).wait_send()
            y_copy(d, i).wait()

    each(finish)
    x_side_own().wait_send()


def solution(mesh):
    assert mesh.shape["tp"] == 2 * RING

    def step(x, w_gate, w_up, w_down):
        rows, dim = x.shape
        ff = w_gate.shape[1]
        n = RING
        chunks = rows // 2 // CHUNK
        hbm = pl.BlockSpec(memory_space=pl.ANY)
        dma = pltpu.SemaphoreType.DMA
        outs = pl.pallas_call(
            kernel,
            out_shape=[
                jax.ShapeDtypeStruct((rows, dim), BF16),
                jax.ShapeDtypeStruct((n, 2, rows, dim), BF16),
                jax.ShapeDtypeStruct((n + 1, rows, dim), BF16),
                jax.ShapeDtypeStruct((n + 1, 2, rows, dim), BF16),
                jax.ShapeDtypeStruct((2 * rows, ff), BF16),
            ],
            in_specs=[hbm] * 4,
            out_specs=[hbm] * 5,
            scratch_shapes=[
                pltpu.VMEM((dim, 2 * ff), BF16),
                pltpu.VMEM((ff, dim), BF16),
                pltpu.VMEM((2 * rows, dim), BF16),
                pltpu.VMEM((rows, dim), F32),
                pltpu.VMEM((rows, N1), F32),
                pltpu.VMEM((2 * rows, ff), BF16),
                pltpu.VMEM((2, rows, dim), BF16),
                dma((4 * ff // N1 + 1,)),
                dma((2,)),
                dma,
                dma((2, 2)),
                dma((n, 3, 2, chunks)),
                dma((n, 2, chunks)),
                dma((n, 2, chunks)),
                dma((n, 2, chunks)),
                dma,
                dma((n + 1,)),
                dma((n + 1, 2, chunks)),
                dma((n + 1, 2, 2, chunks)),
            ],
            compiler_params=pltpu.CompilerParams(
                collective_id=0, has_side_effects=True, vmem_limit_bytes=67043328
            ),
        )(x, w_gate, w_up, w_down)
        return outs[0]

    return jax.shard_map(
        step,
        mesh=mesh,
        in_specs=(P(("dp", "tp"), None), P(None, "tp"), P(None, "tp"), P("tp", None)),
        out_specs=P(("dp", "tp"), None),
        check_vma=False,
    )
```
